32 devices in a mesh: dp: 4 (over x, core), rollout: 8 (over z, y).
Axes of the slice: x: 2, y: 2, z: 4, core: 2. Of those that a mesh axis runs over, the one named last changes fastest.
Arguments:
- queries: bfloat16 [32, 512, 2560], P(('dp', 'rollout')), may hold values from -100 to 100
- resp_keys: bfloat16 [32, 512, 512], P(('dp', 'rollout')), may hold values from -5 to 5
- resp_values: bfloat16 [32, 512, 512], P(('dp', 'rollout')), may hold values from -6 to 6
- prompt_keys: bfloat16 [4, 128, 512], P('dp', 'rollout'), may hold values from -6 to 6
- prompt_values: bfloat16 [4, 128, 512], P('dp', 'rollout'), may hold values from -6 to 6
- d_out: bfloat16 [32, 512, 2560], P(('dp', 'rollout')), may hold values from -6 to 6
- lengths: int32 [32], replicated, may hold values from 64 to 512
- owner: int32 [32], replicated, may hold values from 0 to 3
Outputs:
- attn_out: bfloat16 [32, 512, 2560], P(('dp', 'rollout'))
- d_queries: bfloat16 [32, 512, 2560], P(('dp', 'rollout'))
- d_resp_keys: bfloat16 [32, 512, 512], P(('dp', 'rollout'))
- d_resp_values: bfloat16 [32, 512, 512], P(('dp', 'rollout'))
- d_prompt_keys: float32 [4, 128, 512], P('dp', 'rollout')
- d_prompt_values: float32 [4, 128, 512], P('dp', 'rollout')
The draws below stay inside these ranges and needn't reach their ends.
Inputs may be any that keep to these rules, and one draw needn't show every extreme that they name: `lengths`: rows of a block at or past its length are padding.
All inputs are finite; a program needn't handle non-finite values.
Results may differ from the reference program's by a relative error of at most 0.0071.
Values may be sent and summed in bfloat16 or wider, within the bound.
A program may use at most 128 MiB of HBM per device.

```python
import jax
import jax.numpy as jnp
from jax import lax

HEAD_DIM = 128
BLOCK = 512
TILE = 128
QW = 2560
KW = 512
PROMPT = 128
NB = 32
N_DP = 4


def twin_keys(key):
    base = jax.random.normal(jax.random.fold_in(key, 11), (NB, BLOCK, KW), jnp.float32)
    base = jnp.clip(base, -4.0, 4.0)
    return base


def draw_resp_keys(key, part):
    return twin_keys(key).astype(jnp.bfloat16)


def draw_queries(key, part):
    base = jnp.clip(jax.random.normal(jax.random.fold_in(key, 23), (NB, BLOCK, QW), jnp.float32), -6.0, 6.0)
    return base.astype(jnp.bfloat16)


def touch_ends(entries, rng, least, top_value):
    place = [jax.random.randint(jax.random.fold_in(rng, axis), (), 0, length) for axis, length in enumerate(entries.shape)]
    longest = entries.shape.index(max(entries.shape))
    next_to = place[:longest] + [(place[longest] + 1) % entries.shape[longest]] + place[longest + 1:]
    return entries.at[tuple(place)].set(least).at[tuple(next_to)].set(top_value)


def levels(own_key, shape, shards, low, high):
    def one(position, parts):
        draws = jax.random.uniform(jax.random.fold_in(jax.random.fold_in(own_key, 6), position), (parts,), jnp.float32, low / len(shards), high / len(shards))
        return jnp.repeat(jnp.exp(draws), shape[position] // parts).reshape((-1,) + (1,) * (len(shape) - position - 1))

    level = one(*shards[0])
    for cut in shards[1:]:
        level = level * one(*cut)
    return level


def scatter_about(own_key, shape, width, most, split=(), kind=jnp.bfloat16):
    array = jax.random.normal(own_key, shape, jnp.float32) * width
    if len(split) > 0:
        array = levels(own_key, shape, split, -0.22, 0.18) * array
    return jnp.clip(array, min=-most, max=most).astype(kind)


def setup_inputs(seed: int = 0) -> dict:
    splits = jax.random.split(jax.random.key(seed), 9)
    queries = draw_queries(jax.random.fold_in(splits[8], 71), 0)
    resp_keys = draw_resp_keys(jax.random.fold_in(splits[8], 71), 0)
    resp_values = scatter_about(splits[2], (NB, BLOCK, KW), 1.0, 6.0, ((0, 32),))
    prompt_keys = scatter_about(splits[3], (N_DP, PROMPT, KW), 1.0, 6.0, ((0, 4), (1, 8)))
    prompt_values = scatter_about(splits[4], (N_DP, PROMPT, KW), 1.0, 6.0, ((0, 4), (1, 8)))
    d_out = scatter_about(splits[5], (NB, BLOCK, QW), 1.0, 6.0, ((0, 32),))
    lengths = touch_ends(jax.random.randint(splits[6], (NB,), BLOCK // 8, BLOCK + 1), jax.random.fold_in(splits[6], 1), BLOCK // 8, BLOCK).astype(jnp.int32)
    owner = touch_ends(jax.random.randint(splits[7], (NB,), 0, N_DP), jax.random.fold_in(splits[7], 1), 0, N_DP - 1).astype(jnp.int32)
    return dict(queries=queries, resp_keys=resp_keys, resp_values=resp_values, prompt_keys=prompt_keys, prompt_values=prompt_values, d_out=d_out, lengths=lengths, owner=owner)


def attend(q_rows, d_rows, offset, stride, length, keys, values):
    rows = q_rows.shape[0]
    span = keys.shape[0]
    kv_heads = keys.shape[1] // HEAD_DIM
    group = q_rows.shape[1] // keys.shape[1]
    key_heads = keys.astype(jnp.float32).reshape(span, kv_heads, HEAD_DIM)
    val_heads = values.astype(jnp.float32).reshape(span, kv_heads, HEAD_DIM)
    key_pos = jnp.arange(span, dtype=jnp.int32) - (span - BLOCK)
    live_rows = jnp.clip((length - offset + stride - 1) // stride, 0, rows)
    turns = ((live_rows + TILE - 1) // TILE).astype(jnp.int32)
    scale = HEAD_DIM ** -0.5

    def step(turn, carry):
        out_all, dq_all, dk_sum, dv_sum = carry
        start = (turn * TILE).astype(jnp.int32)
        qt = lax.dynamic_slice_in_dim(q_rows, start, TILE, 0).astype(jnp.float32)
        qt = qt.reshape(TILE, kv_heads, group, HEAD_DIM)
        dt = lax.dynamic_slice_in_dim(d_rows, start, TILE, 0)
        pos = offset + stride * (start + jnp.arange(TILE, dtype=jnp.int32))
        live = pos < length
        dt = jnp.where(live[:, None], dt, jnp.zeros_like(dt))
        dt = dt.astype(jnp.float32).reshape(TILE, kv_heads, group, HEAD_DIM)
        scores = jnp.einsum("tkgd,skd->kgts", qt, key_heads) * scale
        allowed = key_pos[None, :] <= pos[:, None]
        scores = jnp.where(allowed, scores, -1e30)
        top = jnp.max(scores, axis=-1, keepdims=True)
        expd = jnp.exp(scores - top)
        probs = expd / jnp.sum(expd, axis=-1, keepdims=True)
        weights = lax.optimization_barrier(probs.astype(jnp.bfloat16)).astype(jnp.float32)
        out = jnp.einsum("kgts,skd->tkgd", weights, val_heads)
        out = out * live.astype(jnp.float32)[:, None, None, None]
        dprob = jnp.einsum("tkgd,skd->kgts", dt, val_heads)
        delta = jnp.einsum("tkgd,tkgd->kgt", dt, out)
        dscore = probs * (dprob - delta[..., None]) * scale
        dscore = lax.optimization_barrier(dscore.astype(jnp.bfloat16)).astype(jnp.float32)
        dq = jnp.einsum("kgts,skd->tkgd", dscore, key_heads)
        dk_sum = dk_sum + jnp.einsum("kgts,tkgd->skd", dscore, qt)
        dv_sum = dv_sum + jnp.einsum("kgts,tkgd->skd", weights, dt)
        out_all = lax.dynamic_update_slice_in_dim(out_all, out.reshape(TILE, -1).astype(jnp.bfloat16), start, 0)
        dq_all = lax.dynamic_update_slice_in_dim(dq_all, dq.reshape(TILE, -1).astype(jnp.bfloat16), start, 0)
        return out_all, dq_all, dk_sum, dv_sum

    init = (jnp.zeros((rows, q_rows.shape[1]), jnp.bfloat16),
            jnp.zeros((rows, q_rows.shape[1]), jnp.bfloat16),
            jnp.zeros((span, kv_heads, HEAD_DIM), jnp.float32),
            jnp.zeros((span, kv_heads, HEAD_DIM), jnp.float32))
    out_all, dq_all, dk_sum, dv_sum = lax.fori_loop(jnp.int32(0), turns, step, init)
    return out_all, dq_all, dk_sum.reshape(span, -1), dv_sum.reshape(span, -1)


def reference(queries, resp_keys, resp_values, prompt_keys, prompt_values, d_out, lengths, owner):
    groups = prompt_keys.shape[0]
    prompt_n = prompt_keys.shape[1]
    width_k = prompt_keys.shape[2]

    def one(accum, index):
        own = owner[index]
        pkeys = lax.dynamic_index_in_dim(prompt_keys, own, 0, keepdims=False)
        pvals = lax.dynamic_index_in_dim(prompt_values, own, 0, keepdims=False)
        keys = jnp.concatenate([pkeys, resp_keys[index]], axis=0)
        values = jnp.concatenate([pvals, resp_values[index]], axis=0)
        out, dq, dk, dv = attend(queries[index], d_out[index], 0, 1, lengths[index], keys, values)
        select = (jnp.arange(groups, dtype=jnp.int32) == own).astype(jnp.float32)
        term = jnp.concatenate([dk[:prompt_n], dv[:prompt_n]], axis=1)
        accum = accum + select[:, None, None] * term[None]
        return accum, (out, dq, dk[prompt_n:].astype(jnp.bfloat16), dv[prompt_n:].astype(jnp.bfloat16))

    start = jnp.zeros((groups, prompt_n, 2 * width_k), jnp.float32)
    accum, results = lax.scan(one, start, jnp.arange(queries.shape[0], dtype=jnp.int32))
    return results[0], results[1], results[2], results[3], accum[..., :width_k], accum[..., width_k:]
```

```python
import functools
import math

import jax
import jax.numpy as jnp
from jax import lax
from jax.experimental import pallas as pl
from jax.experimental.pallas import tpu as pltpu
from jax.sharding import PartitionSpec as P

HEAD_DIM = 128
MESH = pl.DeviceIdType.MESH
ROWS = 256
VMEM = pltpu.VMEM


def remote(src, dst, send, recv, axis, peer):
    return pltpu.make_async_remote_copy(
        src_ref=src, dst_ref=dst, send_sem=send, recv_sem=recv,
        device_id={axis: peer}, device_id_type=MESH,
    )


def dot(a, b, dims=((1,), (0,))):
    return lax.dot_general(a, b, (dims, ((), ())), preferred_element_type=jnp.float32)


def lanes(e, width):
    return pl.ds(pl.multiple_of(e * width, width), width)


def step_kernel(groups, shards, heads, group,
                owner, lengths, q, d, rk, rv, pk, pv,
                out, dq, dk, dv, dpk, dpv, *scratch):
    held = scratch[:heads]
    (kv, kt, vt, qs, gs, stage, term, got, acc, stage2, got2, dks, dvs,
     lp, lq, s1, r1, s2, r2, s3, r3, s4, r4) = scratch[heads:]
    dp, ro = lax.axis_index("dp"), lax.axis_index("rollout")
    block = q.shape[1]
    span = kv.shape[2]
    pn = span - block
    n = pn // shards
    width = group * HEAD_DIM
    scale = HEAD_DIM ** -0.5
    live_n = lengths[dp * shards + ro]
    row = pl.ds(pl.multiple_of(ro * n, n), n)

    def rows_for(peer):
        return pl.ds(pl.multiple_of(peer * n, n), n)

    barrier = pltpu.get_barrier_semaphore()
    for k in range(1, groups):
        pl.semaphore_signal(
            barrier, inc=1, device_id={"dp": lax.rem(dp + k, groups)}, device_id_type=MESH
        )
    for k in range(1, shards):
        pl.semaphore_signal(
            barrier, inc=1, device_id={"rollout": lax.rem(ro + k, shards)}, device_id_type=MESH
        )

    def prompt_loads(e):
        cols = pl.ds(e * HEAD_DIM, HEAD_DIM)
        return [
            pltpu.make_async_copy(pk.at[0, :, cols], held[e].at[0, 0], lp.at[e, 0]),
            pltpu.make_async_copy(pv.at[0, :, cols], held[e].at[0, 1], lp.at[e, 1]),
        ]

    def loads(e):
        cols = lanes(e, HEAD_DIM)
        wide = lanes(e, width)
        return [
            pltpu.make_async_copy(rk.at[0, :, cols], kv.at[e, 0, pl.ds(pn, block), :], lq.at[e, 0]),
            pltpu.make_async_copy(q.at[0, :, wide], qs.at[e], lq.at[e, 1]),
            pltpu.make_async_copy(rv.at[0, :, cols], kv.at[e, 1, pl.ds(pn, block), :], lq.at[e, 2]),
            pltpu.make_async_copy(d.at[0, :, wide], gs.at[e], lq.at[e, 3]),
        ]

    for e in range(heads):
        for copy in prompt_loads(e):
            copy.start()
    for e in range(heads):
        for copy in loads(e):
            copy.start()
    for e in range(heads):
        for copy in prompt_loads(e):
            copy.wait()
    pl.semaphore_wait(barrier, groups + shards - 2)

    def gather1(e, k):
        return remote(held[e].at[0], held[e].at[k], s1.at[e, k], r1.at[e, k],
                      "dp", lax.rem(dp + k, groups))

    def gather2(e, k):
        return remote(stage.at[e, k], kv.at[e, :, row, :], s2.at[e, k], r2.at[e, k],
                      "rollout", lax.rem(ro + k, shards))

    def reduce1(e, k):
        peer = lax.rem(ro + k, shards)
        return remote(term.at[e, :, rows_for(peer), :], got.at[e, k], s3.at[e, k], r3.at[e, k],
                      "rollout", peer)

    def reduce2(e, k):
        return remote(stage2.at[e, k], got2.at[e, k], s4.at[e, k], r4.at[e, k],
                      "dp", lax.rem(dp + k, groups))

    for e in range(heads):
        for k in range(1, groups):
            gather1(e, k).start()
    for e in range(heads):
        for k in range(1, groups):
            gather1(e, k).wait_recv()

        def rows_of(peer):
            return held[e][lax.rem(dp - owner[dp * shards + peer] + groups, groups)]

        for k in range(1, shards):
            stage[e, k] = rows_of(lax.rem(ro + k, shards))
            gather2(e, k).start()
        kv[e, :, row, :] = rows_of(ro)

    lead = lax.broadcasted_iota(jnp.int32, (ROWS, ROWS), 0) <= lax.broadcasted_iota(
        jnp.int32, (ROWS, ROWS), 1
    )
    c = scale * math.log2(math.e)

    def compute(e):
        kc, vc = kv.at[e, 0], kv.at[e, 1]
        kt[...] = kc[...].T
        vt[...] = vc[...].T
        dks[...] = jnp.zeros_like(dks)
        dvs[...] = jnp.zeros_like(dvs)

        def head(h):
            cols = pl.ds(h * HEAD_DIM, HEAD_DIM)
            at = pl.ds(pl.multiple_of(e * width + h * HEAD_DIM, HEAD_DIM), HEAD_DIM)
            for t in range(block // ROWS):
                rows = pl.ds(t * ROWS, ROWS)
                old, end = pn + t * ROWS, pn + (t + 1) * ROWS
                live = (
                    lax.broadcasted_iota(jnp.int32, (ROWS, HEAD_DIM), 0) + t * ROWS < live_n
                )
                qt = qs[e, rows, cols]
                g = jnp.where(live, gs[e, rows, cols].astype(jnp.float32), 0.0).astype(jnp.bfloat16)
                sa = dot(kc[:old], qt, ((1,), (1,))) * c
                sb = jnp.where(lead, dot(kc[old:end], qt, ((1,), (1,))) * c, -1e30)
                top = jnp.maximum(
                    jnp.max(sa, axis=0, keepdims=True), jnp.max(sb, axis=0, keepdims=True)
                )
                ea, eb = jnp.exp2(sa - top), jnp.exp2(sb - top)
                inv = 1.0 / (
                    jnp.sum(ea, axis=0, keepdims=True) + jnp.sum(eb, axis=0, keepdims=True)
                )
                p = jnp.concatenate([ea, eb], axis=0) * inv
                w = p.astype(jnp.bfloat16)
                o = dot(vt[:, :end], w)
                out[0, rows, at] = jnp.where(live, o.T, 0.0).astype(jnp.bfloat16)
                dpr = dot(vc[:end], g, ((1,), (1,)))
                delta = jnp.sum(p * dpr, axis=0, keepdims=True)
                ds = (p * (dpr - delta)).astype(jnp.bfloat16)
                dq[0, rows, at] = (dot(kt[:, :end], ds) * scale).T.astype(jnp.bfloat16)
                dks[:end] += dot(ds, qt)
                dvs[:end] += dot(w, g)

        for h in range(group):
            head(h)
        dkf = dks[...] * scale
        narrow = lanes(e, HEAD_DIM)
        dk[0, :, narrow] = dkf[pn:].astype(jnp.bfloat16)
        dv[0, :, narrow] = dvs[pn:].astype(jnp.bfloat16)
        term[e, 0] = dkf[:pn].astype(jnp.bfloat16)
        term[e, 1] = dvs[:pn].astype(jnp.bfloat16)

    def collect(e):
        for k in range(1, shards):
            reduce1(e, k).wait_recv()
        got[e, 0] = term[e, :, row, :]
        for k in range(groups):
            target = lax.rem(dp + k, groups)
            total = jnp.zeros(acc.shape[1:], jnp.float32)
            for j in range(shards):
                source = lax.rem(ro - j + shards, shards)
                pick = (owner[dp * shards + source] == target).astype(jnp.float32)
                total = total + pick * got[e, j].astype(jnp.float32)
            if k == 0:
                acc[e] = total
            else:
                stage2[e, k] = total.astype(jnp.bfloat16)
                reduce2(e, k).start()

    def turn(e, carry):
        for copy in loads(e):
            copy.wait()
        for k in range(1, shards):
            gather2(e, k).wait_recv()
        compute(e)
        for k in range(1, shards):
            reduce1(e, k).start()

        @pl.when(e > 0)
        def _():
            collect(e - 1)

        return carry

    lax.fori_loop(0, heads, turn, 0)
    collect(heads - 1)
    for e in range(heads):
        cols = pl.ds(e * HEAD_DIM, HEAD_DIM)
        for k in range(1, groups):
            reduce2(e, k).wait_recv()
        total = acc[e]
        for k in range(1, groups):
            total = total + got2[e, k].astype(jnp.float32)
        dpk[0, :, cols] = total[0]
        dpv[0, :, cols] = total[1]
    for e in range(heads):
        for k in range(1, groups):
            gather1(e, k).wait_send()
            reduce2(e, k).wait_send()
        for k in range(1, shards):
            gather2(e, k).wait_send()
            reduce1(e, k).wait_send()


def flush_kernel(count, *refs):
    sems = refs[-1]
    copies = [pltpu.make_async_copy(refs[i], refs[count + i], sems.at[i]) for i in range(count)]
    for copy in copies:
        copy.start()
    for copy in copies:
        copy.wait()


def per_device(queries, resp_keys, resp_values, prompt_keys, prompt_values, d_out, lengths, owner):
    shards = lax.axis_size("rollout")
    groups = lax.axis_size("dp")
    n, kw = prompt_keys.shape[1:]
    pn = n * shards
    block, qw = queries.shape[1:]
    heads = kw // HEAD_DIM
    group = qw // kw
    span = pn + block
    smem = pl.BlockSpec(memory_space=pltpu.SMEM)
    vmem = pl.BlockSpec(memory_space=pltpu.VMEM)
    anyw = pl.BlockSpec(memory_space=pltpu.HBM)
    dma = pltpu.SemaphoreType.DMA
    bf16, f32 = jnp.bfloat16, jnp.float32
    shapes = [(queries.shape, bf16), (queries.shape, bf16), (resp_keys.shape, bf16),
              (resp_keys.shape, bf16), (prompt_keys.shape, f32), (prompt_keys.shape, f32)]
    results = pl.pallas_call(
        functools.partial(step_kernel, groups, shards, heads, group),
        out_shape=tuple(VMEM(s, t) for s, t in shapes),
        in_specs=[smem, smem] + [anyw] * 6,
        out_specs=(vmem,) * 6,
        scratch_shapes=[VMEM((groups, 2, n, HEAD_DIM), bf16)] * heads + [
            VMEM((heads, 2, span, HEAD_DIM), bf16),
            VMEM((HEAD_DIM, span), bf16), VMEM((HEAD_DIM, span), bf16),
            VMEM((heads, block, group * HEAD_DIM), bf16),
            VMEM((heads, block, group * HEAD_DIM), bf16),
            VMEM((heads, shards, 2, n, HEAD_DIM), bf16),
            VMEM((heads, 2, pn, HEAD_DIM), bf16),
            VMEM((heads, shards, 2, n, HEAD_DIM), bf16),
            VMEM((heads, 2, n, HEAD_DIM), f32),
            VMEM((heads, groups, 2, n, HEAD_DIM), bf16),
            VMEM((heads, groups, 2, n, HEAD_DIM), bf16),
            VMEM((span, HEAD_DIM), f32), VMEM((span, HEAD_DIM), f32),
            dma((heads, 2)), dma((heads, 4)),
            dma((heads, groups)), dma((heads, groups)), dma((heads, shards)), dma((heads, shards)),
            dma((heads, shards)), dma((heads, shards)), dma((heads, groups)), dma((heads, groups)),
        ],
        compiler_params=pltpu.CompilerParams(
            collective_id=0, has_side_effects=True, vmem_limit_bytes=48 * 1024 * 1024
        ),
        name="attend",
    )(owner, lengths, *(pltpu.with_memory_space_constraint(x, pltpu.HBM) for x in (
        queries, d_out, resp_keys, resp_values, prompt_keys, prompt_values)))
    return pl.pallas_call(
        functools.partial(flush_kernel, len(shapes)),
        out_shape=tuple(jax.ShapeDtypeStruct(s, t) for s, t in shapes),
        in_specs=[vmem] * len(shapes),
        out_specs=(anyw,) * len(shapes),
        scratch_shapes=[dma((len(shapes),))],
        compiler_params=pltpu.CompilerParams(vmem_limit_bytes=1024 * 1024),
        name="flush",
    )(*results)


def solution(mesh):
    rows = P(("dp", "rollout"), None, None)
    prompt = P("dp", "rollout", None)
    return jax.shard_map(
        per_device,
        mesh=mesh,
        in_specs=(rows, rows, rows, prompt, prompt, rows, P(), P()),
        out_specs=(rows, rows, rows, rows, prompt, prompt),
        check_vma=False,
    )
```

```python
import functools
import math

import jax
import jax.numpy as jnp
from jax import lax
from jax.experimental import pallas as pl
from jax.experimental.pallas import tpu as pltpu
from jax.sharding import PartitionSpec as P

HEAD_DIM = 128
MESH = pl.DeviceIdType.MESH
ROWS = 256
VMEM = pltpu.VMEM


def remote(src, dst, send, recv, axis, peer):
    return pltpu.make_async_remote_copy(
        src_ref=src, dst_ref=dst, send_sem=send, recv_sem=recv,
        device_id={axis: peer}, device_id_type=MESH,
    )


def dot(a, b, dims=((1,), (0,))):
    return lax.dot_general(a, b, (dims, ((), ())), preferred_element_type=jnp.float32)


def lanes(e, width):
    return pl.ds(pl.multiple_of(e * width, width), width)


def step_kernel(groups, shards, heads, group,
                owner, lengths, q, d, rk, rv, pk, pv,
                out, dq, dk, dv, dpk, dpv, *scratch):
    held = scratch[:heads]
    turns = q.shape[1] // ROWS
    dss, ws, sr, dr = (scratch[heads + i * turns:heads + (i + 1) * turns] for i in range(4))
    (kv, kt, vt, qs, gs, stage, term, got, acc, stage2, got2, dks, dvs,
     gsc, qsc, sp, wp, tops, sums, ex,
     lp, lq, s1, r1, s2, r2, s3, r3, s4, r4) = scratch[heads + 4 * turns:]
    dp, ro = lax.axis_index("dp"), lax.axis_index("rollout")
    block = q.shape[1]
    span = kv.shape[2]
    pn = span - block
    n = pn // shards
    width = group * HEAD_DIM
    scale = HEAD_DIM ** -0.5
    live_n = lengths[dp * shards + ro]
    row = pl.ds(pl.multiple_of(ro * n, n), n)

    def rows_for(peer):
        return pl.ds(pl.multiple_of(peer * n, n), n)

    barrier = pltpu.get_barrier_semaphore()
    for k in range(1, groups):
        pl.semaphore_signal(
            barrier, inc=1, device_id={"dp": lax.rem(dp + k, groups)}, device_id_type=MESH
        )
    for k in range(1, shards):
        pl.semaphore_signal(
            barrier, inc=1, device_id={"rollout": lax.rem(ro + k, shards)}, device_id_type=MESH
        )

    def prompt_loads(e):
        cols = pl.ds(e * HEAD_DIM, HEAD_DIM)
        return [
            pltpu.make_async_copy(pk.at[0, :, cols], held[e].at[0, 0], lp.at[e, 0]),
            pltpu.make_async_copy(pv.at[0, :, cols], held[e].at[0, 1], lp.at[e, 1]),
        ]

    def loads(e, i):
        own, wide = (rk, q) if i == 0 else (rv, d)
        whole = qs if i == 0 else gs
        return [
            pltpu.make_async_copy(
                own.at[0, :, lanes(e, HEAD_DIM)], kv.at[e, i, pl.ds(pn, block), :], lq.at[e, 2 * i]
            ),
            pltpu.make_async_copy(
                wide.at[0, :, lanes(e, width)], whole.at[e], lq.at[e, 2 * i + 1]
            ),
        ]

    for e in range(heads):
        for copy in prompt_loads(e):
            copy.start()
    for e in range(heads):
        for i in range(2):
            for copy in loads(e, i):
                copy.start()

    def gather1(e, k):
        return remote(held[e].at[0], held[e].at[k], s1.at[e, k], r1.at[e, k],
                      "dp", lax.rem(dp + k, groups))

    def gather2(e, k):
        return remote(stage.at[e, k], kv.at[e, :, row, :], s2.at[e, k], r2.at[e, k],
                      "rollout", lax.rem(ro + k, shards))

    def reduce1(e, k):
        peer = lax.rem(ro + k, shards)
        return remote(term.at[e, :, rows_for(peer), :], got.at[e, k], s3.at[e, k], r3.at[e, k],
                      "rollout", peer)

    def reduce2(e, k):
        return remote(stage2.at[e, k], got2.at[e, k], s4.at[e, k], r4.at[e, k],
                      "dp", lax.rem(dp + k, groups))

    lead = lax.broadcasted_iota(jnp.int32, (ROWS, ROWS), 0) <= lax.broadcasted_iota(
        jnp.int32, (ROWS, ROWS), 1
    )
    c = scale * math.log2(math.e)

    items = [(h, t) for h in range(group) for t in range(turns)]

    def response_part(e):
        for i in range(2):
            for copy in loads(e, i):
                copy.wait()
        peaks = [None] * len(items)

        def scores(i):
            h, t = items[i]
            qt = qs[e, pl.ds(t * ROWS, ROWS), pl.ds(h * HEAD_DIM, HEAD_DIM)]
            old, end = t * ROWS, (t + 1) * ROWS
            sb = jnp.where(lead, dot(kv[e, 0, pn + old:pn + end], qt, ((1,), (1,))), -1e30)
            top = jnp.max(sb, axis=0, keepdims=True)
            sr[t][e * group + h, old:end] = sb
            if t:
                sa = dot(kv[e, 0, pn:pn + old], qt, ((1,), (1,)))
                top = jnp.maximum(top, jnp.max(sa, axis=0, keepdims=True))
                sr[t][e * group + h, :old] = sa
            peaks[i] = top * c
            tops[e, pl.ds(i, 1), :] = peaks[i]

        def powers(i):
            h, t = items[i]
            x = jnp.exp2(sr[t][e * group + h] * c - peaks[i])
            sums[e, pl.ds(i, 1), :] = jnp.sum(x, axis=0, keepdims=True)
            sr[t][e * group + h] = x
            ws[t][e * group + h] = x.astype(jnp.bfloat16)

        def prob_grads(i):
            h, t = items[i]
            rows = pl.ds(t * ROWS, ROWS)
            live = lax.broadcasted_iota(jnp.int32, (ROWS, HEAD_DIM), 0) + t * ROWS < live_n
            g = jnp.where(live, gs[e, rows, pl.ds(h * HEAD_DIM, HEAD_DIM)].astype(jnp.float32), 0.0)
            dr[t][e * group + h] = dot(
                kv[e, 1, pn:pn + (t + 1) * ROWS], g.astype(jnp.bfloat16), ((1,), (1,))
            )

        for s in range(len(items) + 1):
            if s < len(items):
                scores(s)
                if e < heads - 1:
                    prob_grads(s)
            if s:
                powers(s - 1)

    def attend(e, last):
        info = [{} for _ in items]
        kt[...] = kv[e, 0].T
        vt[...] = kv[e, 1].T

        def place(i):
            h, t = items[i]
            cols = pl.ds(h * HEAD_DIM, HEAD_DIM)
            at = pl.ds(pl.multiple_of(e * width + h * HEAD_DIM, HEAD_DIM), HEAD_DIM)
            return h, t, cols, at, pl.ds(t * ROWS, ROWS), (t + 1) * ROWS

        def prompt_scores(i):
            h, t, cols, at, rows, end = place(i)
            s = dot(kv[e, 0, :pn], qs[e, rows, cols], ((1,), (1,)))
            sp[i % 2] = s
            own = tops[e, pl.ds(i, 1), :]
            top = jnp.maximum(jnp.max(s, axis=0, keepdims=True) * c, own)
            info[i]["top"] = top
            info[i]["part"] = jnp.exp2(own - top)

        def weigh(i):
            h, t, cols, at, rows, end = place(i)
            x = jnp.exp2(sp[i % 2] * c - info[i]["top"])
            total = jnp.sum(x, axis=0, keepdims=True) + sums[e, pl.ds(i, 1), :] * info[i]["part"]
            info[i]["inv"] = 1.0 / total
            ex[i % 3] = x
            wp[i % 4] = x.astype(jnp.bfloat16)

        def forward(i):
            h, t, cols, at, rows, end = place(i)
            inv, part = info[i]["inv"], info[i]["part"]
            o = dot(vt[:, :pn], wp[i % 4]) * inv
            o = o + dot(vt[:, pn:pn + end], ws[t][e * group + h]) * (inv * part)
            live = lax.broadcasted_iota(jnp.int32, (HEAD_DIM, ROWS), 1) + t * ROWS < live_n
            gt = jnp.where(live, gs[e, rows, cols].T.astype(jnp.float32), 0.0)
            info[i]["delta"] = jnp.sum(o * gt, axis=0, keepdims=True)
            info[i]["gt"] = gt.astype(jnp.bfloat16)
            out[0, rows, at] = jnp.where(live, o, 0.0).astype(jnp.bfloat16).T
            gi = gt * inv
            qi = qs[e, rows, cols].T.astype(jnp.float32) * (inv * scale)
            gsc[0, h, t] = gi.astype(jnp.bfloat16).T
            qsc[0, h, t] = qi.astype(jnp.bfloat16).T
            gsc[1, h, t] = (gi * part).astype(jnp.bfloat16).T
            qsc[1, h, t] = (qi * part).astype(jnp.bfloat16).T

        def score_grads(i):
            h, t, cols, at, rows, end = place(i)
            delta = info[i]["delta"]
            dpr = dot(kv[e, 1, :pn], info[i]["gt"])
            dss[t][h, :pn] = (ex[i % 3] * (dpr - delta)).astype(jnp.bfloat16)
            if last:
                dpr = dot(kv[e, 1, pn:pn + end], info[i]["gt"])
            else:
                dpr = dr[t][e * group + h]
            x = sr[t][e * group + h] * (dpr - delta)
            dss[t][h, pn:] = x.astype(jnp.bfloat16)

        def query_grads(i):
            h, t, cols, at, rows, end = place(i)
            factor = info[i]["inv"] * scale
            grad = dot(kt[:, :pn], dss[t][h, :pn]) * factor
            grad = grad + dot(kt[:, pn:pn + end], dss[t][h, pn:]) * (factor * info[i]["part"])
            dq[0, rows, at] = grad.astype(jnp.bfloat16).T

        def backward(i):
            h, t, cols, at, rows, end = place(i)
            dks[:pn] += dot(dss[t][h, :pn], qsc[0, h, t])
            dvs[:pn] += dot(wp[i % 4], gsc[0, h, t])
            if not last:
                dks[pn:pn + end] += dot(dss[t][h, pn:], qsc[1, h, t])
                dvs[pn:pn + end] += dot(ws[t][e * group + h], gsc[1, h, t])
                query_grads(i)

        dks[...] = jnp.zeros_like(dks)
        dvs[...] = jnp.zeros_like(dvs)
        stages = ((prompt_scores, 0), (score_grads, 3), (backward, 4), (forward, 2), (weigh, 1))
        for s in range(len(items) + 4):
            for stage_fn, late in stages:
                if 0 <= s - late < len(items):
                    stage_fn(s - late)
        term[e, 0] = dks[:pn].astype(jnp.bfloat16)
        term[e, 1] = dvs[:pn].astype(jnp.bfloat16)
        for k in range(1, shards):
            reduce1(e, k).start()
        narrow = lanes(e, HEAD_DIM)
        if not last:
            dk[0, :, narrow] = dks[pn:].astype(jnp.bfloat16)
            dv[0, :, narrow] = dvs[pn:].astype(jnp.bfloat16)
            return None

        def key_grads(t0):
            sk = sv = 0.0
            for h, t in items:
                if t >= t0:
                    sk = sk + dot(dss[t][h, pl.ds(pn + t0 * ROWS, ROWS)], qsc[1, h, t])
                    sv = sv + dot(ws[t][e * group + h, pl.ds(t0 * ROWS, ROWS)], gsc[1, h, t])
            dk[0, pl.ds(t0 * ROWS, ROWS), narrow] = sk.astype(jnp.bfloat16)
            dv[0, pl.ds(t0 * ROWS, ROWS), narrow] = sv.astype(jnp.bfloat16)

        def rest_a():
            for i in range(len(items)):
                query_grads(i)
            key_grads(0)

        def rest_b():
            for t0 in range(1, turns):
                key_grads(t0)

        return rest_a, rest_b

    def collect(e):
        for k in range(1, shards):
            reduce1(e, k).wait_recv()
        got[e, 0] = term[e, :, row, :]
        for k in range(groups):
            target = lax.rem(dp + k, groups)
            total = jnp.zeros(acc.shape[1:], jnp.float32)
            for j in range(shards):
                source = lax.rem(ro - j + shards, shards)
                pick = (owner[dp * shards + source] == target).astype(jnp.float32)
                total = total + pick * got[e, j].astype(jnp.float32)
            if k == 0:
                acc[e] = total
            else:
                stage2[e, k] = total.astype(jnp.bfloat16)
                reduce2(e, k).start()

    def exchange(e):
        for k in range(1, groups):
            gather1(e, k).wait_recv()

        def rows_of(peer):
            return held[e][lax.rem(dp - owner[dp * shards + peer] + groups, groups)]

        for k in range(1, shards):
            stage[e, k] = rows_of(lax.rem(ro + k, shards))
            gather2(e, k).start()
        kv[e, :, row, :] = rows_of(ro)

    def ready(e):
        for k in range(1, shards):
            gather2(e, k).wait_recv()

    def turn(e, carry):
        ready(e)
        attend(e, False)

        @pl.when(e > 0)
        def _():
            collect(e - 1)

        return carry

    response_part(0)
    for e in range(heads):
        for copy in prompt_loads(e):
            copy.wait()
    pl.semaphore_wait(barrier, groups + shards - 2)
    for e in range(heads):
        for k in range(1, groups):
            gather1(e, k).start()
    cut = heads // 2
    for e in range(1, cut):
        response_part(e)
    for e in range(heads):
        exchange(e)
    for e in range(cut, heads):
        response_part(e)
    final = heads - 1
    lax.fori_loop(0, final, turn, 0)
    ready(final)
    rest_a, rest_b = attend(final, True)
    collect(final - 1)
    rest_a()
    collect(final)
    rest_b()
    for e in range(heads):
        cols = pl.ds(e * HEAD_DIM, HEAD_DIM)
        for k in range(1, groups):
            reduce2(e, k).wait_recv()
        total = acc[e]
        for k in range(1, groups):
            total = total + got2[e, k].astype(jnp.float32)
        dpk[0, :, cols] = total[0]
        dpv[0, :, cols] = total[1]
    for e in range(heads):
        for k in range(1, groups):
            gather1(e, k).wait_send()
            reduce2(e, k).wait_send()
        for k in range(1, shards):
            gather2(e, k).wait_send()
            reduce1(e, k).wait_send()


def flush_kernel(count, *refs):
    sems = refs[-1]
    copies = [pltpu.make_async_copy(refs[i], refs[count + i], sems.at[i]) for i in range(count)]
    for copy in copies:
        copy.start()
    for copy in copies:
        copy.wait()


def per_device(queries, resp_keys, resp_values, prompt_keys, prompt_values, d_out, lengths, owner):
    shards = lax.axis_size("rollout")
    groups = lax.axis_size("dp")
    n, kw = prompt_keys.shape[1:]
    pn = n * shards
    block, qw = queries.shape[1:]
    heads = kw // HEAD_DIM
    group = qw // kw
    span = pn + block
    ends = range(ROWS, block + 1, ROWS)
    smem = pl.BlockSpec(memory_space=pltpu.SMEM)
    vmem = pl.BlockSpec(memory_space=pltpu.VMEM)
    anyw = pl.BlockSpec(memory_space=pltpu.HBM)
    dma = pltpu.SemaphoreType.DMA
    bf16, f32 = jnp.bfloat16, jnp.float32
    shapes = [(queries.shape, bf16), (queries.shape, bf16), (resp_keys.shape, bf16),
              (resp_keys.shape, bf16), (prompt_keys.shape, f32), (prompt_keys.shape, f32)]
    results = pl.pallas_call(
        functools.partial(step_kernel, groups, shards, heads, group),
        out_shape=tuple(VMEM(s, t) for s, t in shapes),
        in_specs=[smem, smem] + [anyw] * 6,
        out_specs=(vmem,) * 6,
        scratch_shapes=[VMEM((groups, 2, n, HEAD_DIM), bf16)] * heads + [
            VMEM((group, pn + t, ROWS), bf16) for t in ends
        ] + [
            VMEM((count * group, t, ROWS), kind)
            for count, kind in ((heads, bf16), (heads, f32), (heads - 1, f32)) for t in ends
        ] + [
            VMEM((heads, 2, span, HEAD_DIM), bf16),
            VMEM((HEAD_DIM, span), bf16), VMEM((HEAD_DIM, span), bf16),
            VMEM((heads, block, group * HEAD_DIM), bf16),
            VMEM((heads, block, group * HEAD_DIM), bf16),
            VMEM((heads, shards, 2, n, HEAD_DIM), bf16),
            VMEM((heads, 2, pn, HEAD_DIM), bf16),
            VMEM((heads, shards, 2, n, HEAD_DIM), bf16),
            VMEM((heads, 2, n, HEAD_DIM), f32),
            VMEM((heads, groups, 2, n, HEAD_DIM), bf16),
            VMEM((heads, groups, 2, n, HEAD_DIM), bf16),
            VMEM((span, HEAD_DIM), f32), VMEM((span, HEAD_DIM), f32),
            VMEM((2, group, len(ends), ROWS, HEAD_DIM), bf16),
            VMEM((2, group, len(ends), ROWS, HEAD_DIM), bf16),
            VMEM((2, pn, ROWS), f32), VMEM((4, pn, ROWS), bf16),
            VMEM((heads, group * len(ends), ROWS), f32),
            VMEM((heads, group * len(ends), ROWS), f32),
            VMEM((3, pn, ROWS), f32),
            dma((heads, 2)), dma((heads, 4)),
            dma((heads, groups)), dma((heads, groups)), dma((heads, shards)), dma((heads, shards)),
            dma((heads, shards)), dma((heads, shards)), dma((heads, groups)), dma((heads, groups)),
        ],
        compiler_params=pltpu.CompilerParams(
            collective_id=0, has_side_effects=True, vmem_limit_bytes=60_600_000
        ),
        name="attend",
    )(owner, lengths, *(pltpu.with_memory_space_constraint(x, pltpu.HBM) for x in (
        queries, d_out, resp_keys, resp_values, prompt_keys, prompt_values)))
    return pl.pallas_call(
        functools.partial(flush_kernel, len(shapes)),
        out_shape=tuple(jax.ShapeDtypeStruct(s, t) for s, t in shapes),
        in_specs=[vmem] * len(shapes),
        out_specs=(anyw,) * len(shapes),
        scratch_shapes=[dma((len(shapes),))],
        compiler_params=pltpu.CompilerParams(vmem_limit_bytes=1024 * 1024),
        name="flush",
    )(*results)


def solution(mesh):
    rows = P(("dp", "rollout"), None, None)
    prompt = P("dp", "rollout", None)
    return jax.shard_map(
        per_device,
        mesh=mesh,
        in_specs=(rows, rows, rows, prompt, prompt, rows, P(), P()),
        out_specs=(rows, rows, rows, rows, prompt, prompt),
        check_vma=False,
    )
```
